32 devices in a mesh: rows: 4 (over y, core), cols: 8 (over z, x).
Axes of the slice: x: 2, y: 2, z: 4, core: 2. Of those that a mesh axis runs over, the one named last changes fastest.
Arguments:
- terrain_grid: float32 [4096, 4096], P('rows', 'cols'), may hold values from -360 to 360
Outputs:
- shade: float32 [4096, 4096], P('rows', 'cols')
- first: float32 [2048, 2048], P('rows', 'cols')
- second: float32 [1024, 1024], P('rows', 'cols')
- third: float32 [512, 512], P('rows', 'cols')
The draws below stay inside these ranges and needn't reach their ends.
All inputs are finite; a program needn't handle non-finite values.
Results may differ from the reference program's by a relative error of at most 0.0003.
Values sent between devices are 32-bit elements; how exact they have to be, the bound alone decides.
A program may use at most 64 MiB of HBM per device.

```python
import math
import jax
import jax.numpy as jnp
from jax import lax

NEIGHBOUR_REACH = 120
NR = 4096
NC = 4096


def draw_terrain_grid(key, part):
    keys = jax.random.split(key, 9)
    row_pos = jnp.arange(NR, dtype=jnp.float32)[:, None]
    col_pos = jnp.arange(NC, dtype=jnp.float32)[None, :]
    terrain = jnp.zeros((NR, NC), jnp.float32)
    cycles_row = jax.random.uniform(keys[0], (6,), jnp.float32, -3.0, 3.0)
    cycles_col = jax.random.uniform(keys[1], (6,), jnp.float32, -3.0, 3.0)
    phases = jax.random.uniform(keys[2], (6,), jnp.float32, 0.0, 2.0 * math.pi)
    heights = jax.random.uniform(keys[3], (6,), jnp.float32, 20.0, 50.0)
    for number in range(6):
        terrain = terrain + heights[number] * jnp.cos(2.0 * math.pi * (cycles_row[number] * row_pos / NR + cycles_col[number] * col_pos / NC) + phases[number])
    lengths = jnp.exp(jax.random.uniform(keys[4], (8,), jnp.float32, math.log(2.0 * NEIGHBOUR_REACH), math.log(8.0 * NEIGHBOUR_REACH)))
    angles = jax.random.uniform(keys[5], (8,), jnp.float32, -math.pi, math.pi)
    shifts = jax.random.uniform(keys[6], (8,), jnp.float32, 0.0, 2.0 * math.pi)
    ridges = jax.random.uniform(keys[7], (8,), jnp.float32, 2.0, 6.0)
    for number in range(8):
        wave = 2.0 * math.pi / lengths[number]
        terrain = terrain + ridges[number] * jnp.cos(wave * (jnp.cos(angles[number]) * row_pos + jnp.sin(angles[number]) * col_pos) + shifts[number])
    noise = jnp.clip(jax.random.normal(keys[8], (NR, NC), jnp.float32), -5.0, 5.0)
    return terrain + noise


def setup_inputs(seed: int = 0) -> dict:
    streams_of = jax.random.split(jax.random.key(seed), 2)
    return {
        "terrain_grid": draw_terrain_grid(jax.random.fold_in(streams_of[1], 71), 0),
    }


zfactor = 2.0
light_east = -0.5
light_south = -0.5
light_up = math.sqrt(0.5)

def window_extreme(field, count, axis, pick):
    result = field
    power = 1
    while power * 2 <= count:
        length = result.shape[axis] - power
        result = pick(lax.slice_in_dim(result, 0, length, axis=axis), lax.slice_in_dim(result, power, power + length, axis=axis))
        power = power * 2
    rest = count - power
    if rest > 0:
        length = result.shape[axis] - rest
        result = pick(lax.slice_in_dim(result, 0, length, axis=axis), lax.slice_in_dim(result, rest, rest + length, axis=axis))
    return result

def horn_shade(bordered_landform):
    north_west = bordered_landform[:-2, :-2]
    north = bordered_landform[:-2, 1:-1]
    north_east = bordered_landform[:-2, 2:]
    west = bordered_landform[1:-1, :-2]
    east = bordered_landform[1:-1, 2:]
    south_west = bordered_landform[2:, :-2]
    south = bordered_landform[2:, 1:-1]
    south_east = bordered_landform[2:, 2:]
    slope_x = zfactor * (north_east + 2.0 * east + south_east - (north_west + 2.0 * west + south_west)) / 8.0
    slope_y = zfactor * (south_west + 2.0 * south + south_east - (north_west + 2.0 * north + north_east)) / 8.0
    lit = (light_up - light_east * slope_x - light_south * slope_y) / jnp.sqrt(1.0 + slope_x * slope_x + slope_y * slope_y)
    return jnp.maximum(lit, 0.0)

def reduce_level(bordered_landform):
    rows_sum = (bordered_landform[0:-3:2] + 3.0 * bordered_landform[1:-2:2] + 3.0 * bordered_landform[2:-1:2] + bordered_landform[3::2]) / 8.0
    return (rows_sum[:, 0:-3:2] + 3.0 * rows_sum[:, 1:-2:2] + 3.0 * rows_sum[:, 2:-1:2] + rows_sum[:, 3::2]) / 8.0

def reference(terrain_grid):
    bordered_landform = jnp.pad(terrain_grid, NEIGHBOUR_REACH, mode='edge')
    block_rows = math.gcd(NR, 512)
    span = 2 * NEIGHBOUR_REACH + 1

    def rows_block(index):
        piece = lax.dynamic_slice_in_dim(bordered_landform, index * block_rows, block_rows + 2 * NEIGHBOUR_REACH, 0)
        highest = window_extreme(window_extreme(piece, span, 1, jnp.maximum), span, 0, jnp.maximum)
        lowest = window_extreme(window_extreme(piece, span, 1, jnp.minimum), span, 0, jnp.minimum)
        return (highest + lowest) * 0.5
    triangular_filtering = lax.map(rows_block, jnp.arange(NR // block_rows, dtype=jnp.int32))
    triangular_filtering = triangular_filtering.reshape(NR, NC)
    neighbourhood_spread = terrain_grid - triangular_filtering
    shade = horn_shade(jnp.pad(neighbourhood_spread, 1, mode='edge'))
    first = reduce_level(jnp.pad(shade, 1, mode='edge'))
    second = reduce_level(jnp.pad(first, 1, mode='edge'))
    third = reduce_level(jnp.pad(second, 1, mode='edge'))
    return (shade, first, second, third)
```

```python
import math

import jax
import jax.numpy as jnp
from jax import lax
from jax.experimental import pallas as pl
from jax.experimental.pallas import tpu as pltpu
from jax.sharding import PartitionSpec as P

REACH = 120
HALO = 128
LANES = 128
STEPS = 2 * REACH // 8
LIGHT_UP = math.sqrt(0.5)


def rolled(x, k):
    return pltpu.roll(x, x.shape[0] - k, 0)


def group_extremes(load_hi, load_lo, out_hi, out_lo, rows):
    size = 128

    def body(c, carry):
        r = pl.multiple_of(c * size, size)
        top = load_hi(r, size + 8)
        if load_lo is None:
            after = rolled(top, 1)
            hi, lo = jnp.maximum(top, after), jnp.minimum(top, after)
        else:
            low = load_lo(r, size + 8)
            hi, lo = jnp.maximum(top, rolled(top, 1)), jnp.minimum(low, rolled(low, 1))
        for k in (2, 4):
            hi = jnp.maximum(hi, rolled(hi, k))
            lo = jnp.minimum(lo, rolled(lo, k))
        out_hi[pl.ds(r, size), :] = hi[:size]
        out_lo[pl.ds(r, size), :] = lo[:size]
        return carry

    lax.fori_loop(0, rows // size, body, 0)


def window_chunk(load, last, pick, groups):
    held = [None] * groups
    run = load(groups - 1)
    for k in range(groups, STEPS):
        run = pick(run, load(k))
    held[groups - 1] = run
    for g in range(groups - 2, -1, -1):
        run = pick(run, load(g))
        held[g] = run
    out = [pick(held[0], last(STEPS))]
    run = None
    for g in range(1, groups):
        nxt = load(g + STEPS - 1)
        run = nxt if run is None else pick(run, nxt)
        out.append(pick(pick(held[g], run), last(g + STEPS)))
    return out


def chunking(groups):
    return max(g for g in range(1, STEPS) if groups % g == 0)


def vertical_pass(x, vhi, vlo, mhi, mlo, b, rows):
    load = lambda r, n: x[b, pl.ds(r, n), :]
    group_extremes(load, None, mhi, mlo, rows + 2 * HALO)
    total = (rows + 16) // 8
    size = chunking(total)

    def body(c, carry):
        base = c * size
        last = lambda k: x[b, pl.ds(pl.multiple_of((base + k) * 8, 8), 8), :]
        for m, v, pick in ((mhi, vhi, jnp.maximum), (mlo, vlo, jnp.minimum)):
            load = lambda k: m[pl.ds(pl.multiple_of((base + k) * 8, 8), 8), :]
            for g, value in enumerate(window_chunk(load, last, pick, size)):
                v[b, pl.ds(pl.multiple_of((base + g) * 8, 8), 8), :] = value
        return carry

    lax.fori_loop(0, total // size, body, 0)


def horizontal_pass(x, vhi, vlo, relief, thi, tlo, mhi, mlo, mid, rb, strips):
    width = strips * LANES
    r = pl.multiple_of(rb * LANES, LANES)
    for b in range(strips):
        thi[b * LANES : (b + 1) * LANES, :] = vhi[b, pl.ds(r, LANES), :].T
        tlo[b * LANES : (b + 1) * LANES, :] = vlo[b, pl.ds(r, LANES), :].T
    group_extremes(
        lambda s, n: thi[pl.ds(s, n), :], lambda s, n: tlo[pl.ds(s, n), :], mhi, mlo, width
    )
    total = (width - 2 * HALO + 16) // 8
    size = chunking(total)

    def body(c, carry):
        base = c * size
        at = lambda ref: (lambda k: ref[pl.ds(pl.multiple_of((base + k) * 8, 8), 8), :])
        highest = window_chunk(at(mhi), at(thi), jnp.maximum, size)
        lowest = window_chunk(at(mlo), at(tlo), jnp.minimum, size)
        for g in range(size):
            mid[pl.ds(pl.multiple_of(REACH + (base + g) * 8, 8), 8), :] = (
                highest[g] + lowest[g]
            ) * 0.5
        return carry

    lax.fori_loop(0, total // size, body, 0)
    q = pl.multiple_of(r + REACH, 8)
    for b in range(strips):
        relief[b, pl.ds(q, LANES), :] = (
            x[b, pl.ds(q, LANES), :] - mid[b * LANES : (b + 1) * LANES, :].T
        )


def repair(ref, strips, first_row, rows, low, high, edges):
    top, bottom, left, right = edges

    @pl.when(top)
    def _():
        for b in range(strips):
            ref[b, first_row - 8 : first_row, :] = jnp.broadcast_to(
                ref[b, first_row : first_row + 1, :], (8, LANES)
            )

    @pl.when(bottom)
    def _():
        end = first_row + rows
        for b in range(strips):
            ref[b, end : end + 8, :] = jnp.broadcast_to(ref[b, end - 1 : end, :], (8, LANES))

    @pl.when(left)
    def _():
        ref[0, low:high, :] = jnp.broadcast_to(ref[1, low:high, 0:1], (high - low, LANES))

    @pl.when(right)
    def _():
        ref[strips - 1, low:high, :] = jnp.broadcast_to(
            ref[strips - 2, low:high, LANES - 1 : LANES], (high - low, LANES)
        )


def shade_rows(relief, shade, strips, rows):
    size = 16
    width = strips * LANES

    def body(c, carry):
        r = pl.multiple_of(HALO - 16 + c * size, 8)
        wide = jnp.concatenate(
            [relief[b, pl.ds(r - 8, size + 16), :] for b in range(strips)], axis=1
        )
        north = pltpu.roll(wide, 1, 0)[8 : 8 + size]
        south = pltpu.roll(wide, size + 15, 0)[8 : 8 + size]
        here = wide[8 : 8 + size]
        across = north + 2.0 * here + south
        down = south - north
        gx = (pltpu.roll(across, width - 1, 1) - pltpu.roll(across, 1, 1)) * 0.25
        gy = (pltpu.roll(down, width - 1, 1) + 2.0 * down + pltpu.roll(down, 1, 1)) * 0.25
        lit = (LIGHT_UP + 0.5 * gx + 0.5 * gy) * lax.rsqrt(1.0 + gx * gx + gy * gy)
        lit = jnp.maximum(lit, 0.0)
        for b in range(strips):
            shade[b, pl.ds(r, size), :] = lit[:, b * LANES : (b + 1) * LANES]
        return carry

    lax.fori_loop(0, (rows + 32) // size, body, 0)


def tent_matrix(d):
    row = lax.broadcasted_iota(jnp.int32, (LANES, LANES), 0)
    col = lax.broadcasted_iota(jnp.int32, (LANES, LANES), 1)
    t = row + d * LANES - 2 * col + LANES
    near, far = (t == 0) | (t == 1), (t == -1) | (t == 2)
    return jnp.where(near, 0.375, jnp.where(far, 0.125, 0.0)).astype(jnp.bfloat16)


def next_level(source, strips, start, count, outs, uhi, ulo, store):
    def body(b, carry):
        at = lambda k: source[b, pl.ds(2 * start + k, count, stride=2), :]
        u = (at(-1) + at(2)) * 0.125 + (at(0) + at(1)) * 0.375
        upper = u.astype(jnp.bfloat16)
        uhi[b, 0:count, :] = upper
        ulo[b, 0:count, :] = (u - upper.astype(jnp.float32)).astype(jnp.bfloat16)
        return carry

    lax.fori_loop(0, strips, body, 0)
    tents = {d: tent_matrix(d) for d in (-2, -1, 0, 1)}
    for out in outs:
        parts = [b for b in range(2 * out - 2, 2 * out + 2) if 0 <= b < strips]
        weights = jnp.concatenate([tents[b - 2 * out] for b in parts], axis=0)
        total = None
        for u in (uhi, ulo):
            left = jnp.concatenate([u[b, 0:count, :] for b in parts], axis=1)
            term = jnp.dot(left, weights, preferred_element_type=jnp.float32)
            total = term if total is None else total + term
        store(out, total)


def kernel(
    own, left, right, top, bottom, out_shade, out_first, out_second, out_third,
    x, vhi, vlo, relief, shade, first, second, thi, tlo, mhi, mlo, mid, uhi, ulo, sems,
):
    rows, cols = own.shape
    strips = cols // LANES + 2
    i, ni = lax.axis_index("rows"), lax.axis_size("rows")
    j, nj = lax.axis_index("cols"), lax.axis_size("cols")
    edges = (i == 0, i == ni - 1, j == 0, j == nj - 1)
    mine = pl.ds(HALO, rows)
    copies = []
    for b in range(strips - 2):
        copies.append((own.at[:, pl.ds(b * LANES, LANES)], x.at[b + 1, mine, :]))
    copies.append((left, x.at[0, mine, :]))
    copies.append((right, x.at[strips - 1, mine, :]))
    for b in range(strips):
        lanes = pl.ds(b * LANES, LANES)
        copies.append((top.at[:, lanes], x.at[b, pl.ds(0, HALO), :]))
        copies.append((bottom.at[:, lanes], x.at[b, pl.ds(HALO + rows, HALO), :]))
    started = [pltpu.make_async_copy(s, d, sems.at[n]) for n, (s, d) in enumerate(copies)]
    for copy in started:
        copy.start()
    mid[...] = jnp.zeros_like(mid)
    for copy in started:
        copy.wait()

    @pl.when(edges[2])
    def _():
        x[0, 0 : rows + 2 * HALO, :] = jnp.broadcast_to(
            x[1, 0 : rows + 2 * HALO, 0:1], (rows + 2 * HALO, LANES)
        )

    @pl.when(edges[3])
    def _():
        x[strips - 1, 0 : rows + 2 * HALO, :] = jnp.broadcast_to(
            x[strips - 2, 0 : rows + 2 * HALO, LANES - 1 : LANES], (rows + 2 * HALO, LANES)
        )

    @pl.when(edges[0])
    def _():
        for b in range(strips):
            x[b, 0:HALO, :] = jnp.broadcast_to(x[b, HALO : HALO + 1, :], (HALO, LANES))

    @pl.when(edges[1])
    def _():
        end = HALO + rows
        for b in range(strips):
            x[b, end : end + HALO, :] = jnp.broadcast_to(x[b, end - 1 : end, :], (HALO, LANES))

    def down(b, carry):
        vertical_pass(x, vhi, vlo, mhi, mlo, b, rows)
        return carry

    lax.fori_loop(0, strips, down, 0)

    def along(rb, carry):
        horizontal_pass(x, vhi, vlo, relief, thi, tlo, mhi, mlo, mid, rb, strips)
        return carry

    lax.fori_loop(0, rows // LANES + 1, along, 0)

    repair(relief, strips, HALO, rows, HALO - 8, HALO + rows + 8, edges)
    shade_rows(relief, shade, strips, rows)
    repair(shade, strips, HALO, rows, HALO - 8, HALO + rows + 8, edges)
    outgoing = []

    def send(source, target):
        copy = pltpu.make_async_copy(source, target, sems.at[len(outgoing)])
        copy.start()
        outgoing.append(copy)

    for b in range(strips - 2):
        send(shade.at[b + 1, mine, :], out_shade.at[:, pl.ds(b * LANES, LANES)])

    half, quarter = HALO // 2, HALO // 4
    strips1 = cols // 256 + 2
    low = half - 8

    def keep_first(out, value):
        first[out, low : low + rows // 2 + 16, :] = value

    next_level(shade, strips, low, rows // 2 + 16, range(strips1), uhi, ulo, keep_first)
    repair(first, strips1, half, rows // 2, low, low + rows // 2 + 16, edges)
    for b in range(strips1 - 2):
        send(
            first.at[b + 1, pl.ds(half, rows // 2), :],
            out_first.at[:, pl.ds(b * LANES, LANES)],
        )
    strips2 = cols // 512 + 2
    low2 = quarter - 8

    def keep_second(out, value):
        second[out, low2 : low2 + rows // 4 + 16, :] = value

    next_level(first, strips1, low2, rows // 4 + 16, range(strips2), uhi, ulo, keep_second)
    repair(second, strips2, quarter, rows // 4, low2, low2 + rows // 4 + 16, edges)
    for b in range(strips2 - 2):
        send(
            second.at[b + 1, pl.ds(quarter, rows // 4), :],
            out_second.at[:, pl.ds(b * LANES, LANES)],
        )

    def keep_third(out, value):
        n = min(LANES, cols // 8 - (out - 1) * LANES)
        out_third[:, (out - 1) * LANES : (out - 1) * LANES + n] = value[:, :n]

    outs3 = range(1, 1 + -(-cols // 1024))
    next_level(second, strips2, HALO // 8, rows // 8, outs3, uhi, ulo, keep_third)
    for copy in outgoing:
        copy.wait()


def shifted(array, axis, by):
    count = lax.axis_size(axis)
    pairs = [(k, k + by) for k in range(count) if 0 <= k + by < count]
    return lax.ppermute(array, axis, pairs)


def on_device(terrain):
    rows, cols = terrain.shape
    strips = cols // LANES + 2
    left = shifted(terrain[:, cols - HALO :], "cols", 1)
    right = shifted(terrain[:, :HALO], "cols", -1)
    top_mine = shifted(terrain[rows - HALO :], "rows", 1)
    bottom_mine = shifted(terrain[:HALO], "rows", -1)
    ends = jnp.concatenate([left[rows - HALO :], right[rows - HALO :]], axis=1)
    starts = jnp.concatenate([left[:HALO], right[:HALO]], axis=1)
    top_ends = shifted(ends, "rows", 1)
    bottom_ends = shifted(starts, "rows", -1)
    top = jnp.concatenate([top_ends[:, :LANES], top_mine, top_ends[:, LANES:]], axis=1)
    bottom = jnp.concatenate([bottom_ends[:, :LANES], bottom_mine, bottom_ends[:, LANES:]], axis=1)
    f32 = jnp.float32
    tall = rows + 2 * HALO + 8
    anywhere = pl.BlockSpec(memory_space=pl.ANY)
    vmem = pl.BlockSpec(memory_space=pltpu.VMEM)
    return pl.pallas_call(
        kernel,
        out_shape=tuple(
            jax.ShapeDtypeStruct((rows // k, cols // k), f32) for k in (1, 2, 4, 8)
        ),
        in_specs=[anywhere] * 5,
        out_specs=(anywhere, anywhere, anywhere, vmem),
        scratch_shapes=[
            pltpu.VMEM((strips, tall, LANES), f32),
            pltpu.VMEM((strips, rows + LANES, LANES), f32),
            pltpu.VMEM((strips, rows + LANES, LANES), f32),
            pltpu.VMEM((strips, tall, LANES), f32),
            pltpu.VMEM((strips, tall, LANES), f32),
            pltpu.VMEM((cols // 256 + 2, rows // 2 + HALO, LANES), f32),
            pltpu.VMEM((cols // 512 + 2, rows // 4 + HALO, LANES), f32),
            pltpu.VMEM((strips * LANES + 8, LANES), f32),
            pltpu.VMEM((strips * LANES + 8, LANES), f32),
            pltpu.VMEM((max(tall, strips * LANES), LANES), f32),
            pltpu.VMEM((max(tall, strips * LANES), LANES), f32),
            pltpu.VMEM((strips * LANES, LANES), f32),
            pltpu.VMEM((strips, rows // 2 + 16, LANES), jnp.bfloat16),
            pltpu.VMEM((strips, rows // 2 + 16, LANES), jnp.bfloat16),
            pltpu.SemaphoreType.DMA((3 * strips + 8,)),
        ],
        compiler_params=pltpu.CompilerParams(vmem_limit_bytes=58 * 1024 * 1024),
    )(terrain, left, right, top, bottom)


def solution(mesh):
    spec = P("rows", "cols")
    return jax.shard_map(
        on_device, mesh=mesh, in_specs=(spec,), out_specs=(spec,) * 4, check_vma=False
    )
```

```python
import math

import jax
import jax.numpy as jnp
from jax import lax
from jax.experimental import pallas as pl
from jax.experimental.pallas import tpu as pltpu
from jax.sharding import PartitionSpec as P

REACH = 120
HALO = 128
LANES = 128
STEPS = 2 * REACH // 8
LIGHT_UP = math.sqrt(0.5)


def rolled(x, k):
    return pltpu.roll(x, x.shape[0] - k, 0)


def group_extremes(load_hi, load_lo, out_hi, out_lo, rows, size=128):
    def body(c, carry):
        r = pl.multiple_of(c * size, 8)
        top = load_hi(r, size + 8)
        if load_lo is None:
            after = rolled(top, 1)
            hi, lo = jnp.maximum(top, after), jnp.minimum(top, after)
        else:
            low = load_lo(r, size + 8)
            hi, lo = jnp.maximum(top, rolled(top, 1)), jnp.minimum(low, rolled(low, 1))
        for k in (2, 4):
            hi = jnp.maximum(hi, rolled(hi, k))
            lo = jnp.minimum(lo, rolled(lo, k))
        out_hi[pl.ds(r, size), :] = hi[:size]
        out_lo[pl.ds(r, size), :] = lo[:size]
        return carry

    lax.fori_loop(0, rows // size, body, 0)


def window_chunk(load, last, pick, groups):
    held = [None] * groups
    run = load(groups - 1)
    for k in range(groups, STEPS):
        run = pick(run, load(k))
    held[groups - 1] = run
    for g in range(groups - 2, -1, -1):
        run = pick(run, load(g))
        held[g] = run
    out = [pick(held[0], last(STEPS))]
    run = None
    for g in range(1, groups):
        nxt = load(g + STEPS - 1)
        run = nxt if run is None else pick(run, nxt)
        out.append(pick(pick(held[g], run), last(g + STEPS)))
    return out


def chunking(groups):
    return max(g for g in range(1, STEPS) if groups % g == 0)


def vertical_pass(x, vhi, vlo, mhi, mlo, b, rows):
    load = lambda r, n: x[b, pl.ds(r, n), :]
    group_extremes(load, None, mhi, mlo, rows + 2 * HALO)
    total = (rows + 16) // 8
    size = chunking(total)

    def body(c, carry):
        base = c * size
        last = lambda k: x[b, pl.ds(pl.multiple_of((base + k) * 8, 8), 8), :]
        for m, v, pick in ((mhi, vhi, jnp.maximum), (mlo, vlo, jnp.minimum)):
            load = lambda k: m[pl.ds(pl.multiple_of((base + k) * 8, 8), 8), :]
            for g, value in enumerate(window_chunk(load, last, pick, size)):
                v[b, pl.ds(pl.multiple_of((base + g) * 8, 8), 8), :] = value
        return carry

    lax.fori_loop(0, total // size, body, 0)


def halo_pass(x, b, start, vhi, vlo, mhi, mlo):
    row = lambda r: pl.multiple_of(start + r, 8)
    span = LANES + 2 * REACH - 8
    load = lambda r, n: x[b, pl.ds(row(r), n), :]
    group_extremes(load, None, mhi, mlo, span, span // 3)
    last = lambda k: x[b, pl.ds(row(k * 8), 8), :]
    for m, v, pick in ((mhi, vhi, jnp.maximum), (mlo, vlo, jnp.minimum)):
        load = lambda k: m[k * 8 : k * 8 + 8, :]
        for g, value in enumerate(window_chunk(load, last, pick, LANES // 8)):
            v[b, pl.ds(row(g * 8), 8), :] = value


def horizontal_pass(x, vhi, vlo, relief, thi, tlo, mhi, mlo, mid, start, strips):
    width = strips * LANES
    r = pl.multiple_of(start, 8)
    for b in range(strips):
        thi[b * LANES : (b + 1) * LANES, :] = vhi[b, pl.ds(r, LANES), :].T
        tlo[b * LANES : (b + 1) * LANES, :] = vlo[b, pl.ds(r, LANES), :].T
    group_extremes(
        lambda s, n: thi[pl.ds(s, n), :], lambda s, n: tlo[pl.ds(s, n), :], mhi, mlo, width
    )
    total = (width - 2 * HALO + 16) // 8
    size = chunking(total)

    def body(c, carry):
        base = c * size
        at = lambda ref: (lambda k: ref[pl.ds(pl.multiple_of((base + k) * 8, 8), 8), :])
        highest = window_chunk(at(mhi), at(thi), jnp.maximum, size)
        lowest = window_chunk(at(mlo), at(tlo), jnp.minimum, size)
        for g in range(size):
            mid[pl.ds(pl.multiple_of(REACH + (base + g) * 8, 8), 8), :] = (
                highest[g] + lowest[g]
            ) * 0.5
        return carry

    lax.fori_loop(0, total // size, body, 0)
    q = pl.multiple_of(r + REACH, 8)
    for b in range(strips):
        relief[b, pl.ds(q, LANES), :] = (
            x[b, pl.ds(q, LANES), :] - mid[b * LANES : (b + 1) * LANES, :].T
        )


def repair(ref, strips, first_row, rows, low, high, edges):
    top, bottom, left, right = edges

    @pl.when(top)
    def _():
        for b in range(strips):
            ref[b, first_row - 8 : first_row, :] = jnp.broadcast_to(
                ref[b, first_row : first_row + 1, :], (8, LANES)
            )

    @pl.when(bottom)
    def _():
        end = first_row + rows
        for b in range(strips):
            ref[b, end : end + 8, :] = jnp.broadcast_to(ref[b, end - 1 : end, :], (8, LANES))

    @pl.when(left)
    def _():
        ref[0, low:high, :] = jnp.broadcast_to(ref[1, low:high, 0:1], (high - low, LANES))

    @pl.when(right)
    def _():
        ref[strips - 1, low:high, :] = jnp.broadcast_to(
            ref[strips - 2, low:high, LANES - 1 : LANES], (high - low, LANES)
        )


def shade_rows(relief, shade, strips, rows):
    size = 16
    width = strips * LANES

    def body(c, carry):
        r = pl.multiple_of(HALO - 16 + c * size, 8)
        wide = jnp.concatenate(
            [relief[b, pl.ds(r - 8, size + 16), :] for b in range(strips)], axis=1
        )
        north = pltpu.roll(wide, 1, 0)[8 : 8 + size]
        south = pltpu.roll(wide, size + 15, 0)[8 : 8 + size]
        here = wide[8 : 8 + size]
        across = north + 2.0 * here + south
        down = south - north
        gx = (pltpu.roll(across, width - 1, 1) - pltpu.roll(across, 1, 1)) * 0.25
        gy = (pltpu.roll(down, width - 1, 1) + 2.0 * down + pltpu.roll(down, 1, 1)) * 0.25
        lit = (LIGHT_UP + 0.5 * gx + 0.5 * gy) * lax.rsqrt(1.0 + gx * gx + gy * gy)
        lit = jnp.maximum(lit, 0.0)
        for b in range(strips):
            shade[b, pl.ds(r, size), :] = lit[:, b * LANES : (b + 1) * LANES]
        return carry

    lax.fori_loop(0, (rows + 32) // size, body, 0)


def tent_matrix(d):
    row = lax.broadcasted_iota(jnp.int32, (LANES, LANES), 0)
    col = lax.broadcasted_iota(jnp.int32, (LANES, LANES), 1)
    t = row + d * LANES - 2 * col + LANES
    near, far = (t == 0) | (t == 1), (t == -1) | (t == 2)
    return jnp.where(near, 0.375, jnp.where(far, 0.125, 0.0)).astype(jnp.bfloat16)


def next_level(source, strips, start, count, outs, uhi, ulo, store):
    def body(b, carry):
        at = lambda k: source[b, pl.ds(2 * start + k, count, stride=2), :]
        u = (at(-1) + at(2)) * 0.125 + (at(0) + at(1)) * 0.375
        upper = u.astype(jnp.bfloat16)
        uhi[b, 0:count, :] = upper
        ulo[b, 0:count, :] = (u - upper.astype(jnp.float32)).astype(jnp.bfloat16)
        return carry

    lax.fori_loop(0, strips, body, 0)
    tents = {d: tent_matrix(d) for d in (-2, -1, 0, 1)}
    for out in outs:
        parts = [b for b in range(2 * out - 2, 2 * out + 2) if 0 <= b < strips]
        weights = jnp.concatenate([tents[b - 2 * out] for b in parts], axis=0)
        total = None
        for u in (uhi, ulo):
            left = jnp.concatenate([u[b, 0:count, :] for b in parts], axis=1)
            term = jnp.dot(left, weights, preferred_element_type=jnp.float32)
            total = term if total is None else total + term
        store(out, total)


def order_of(chunks):
    order = []
    for k in range(chunks // 2):
        order += [chunks - 1 - k, k]
    return order


def blocks_of(rows):
    chunks = rows // LANES
    order = order_of(chunks)
    starts = [k * LANES for k in range(chunks)] + [rows + 16 - LANES]
    plan = []
    for start in starts:
        low, high = start - HALO, start + LANES + 2 * REACH - HALO
        need = {min(max(c, 0), chunks - 1) for c in range(low // LANES, -(-high // LANES))}
        plan.append((max(2, 1 + max(order.index(c) for c in need)), start))
    return sorted(plan)


def pick_by(step, values):
    result = jnp.int32(values[0])
    for k in range(1, len(values)):
        result = jnp.where(step == k, jnp.int32(values[k]), result)
    return result


def kernel(
    own, out_shade, out_first, out_second, out_third,
    x, vhi, vlo, relief, shade, first, second, thi, tlo, mhi, mlo, mid, uhi, ulo,
    sems, send_side, recv_side, send_row, recv_row, send_end, recv_end,
):
    rows, cols = own.shape
    strips = cols // LANES + 2
    i, ni = lax.axis_index("rows"), lax.axis_size("rows")
    j, nj = lax.axis_index("cols"), lax.axis_size("cols")
    edges = (i == 0, i == ni - 1, j == 0, j == nj - 1)
    has = (i > 0, i < ni - 1, j > 0, j < nj - 1)
    places = ((i - 1, j), (i + 1, j), (i, j - 1), (i, j + 1))
    mine = pl.ds(HALO, rows)
    end = HALO + rows
    chunks = rows // LANES
    order = order_of(chunks)
    MESH = pl.DeviceIdType.MESH

    local = []
    for b in (0, strips - 3, *range(1, strips - 3)):
        copy = pltpu.make_async_copy(
            own.at[:, pl.ds(b * LANES, LANES)], x.at[b + 1, mine, :], sems.at[b]
        )
        copy.start()
        local.append(copy)

    barrier = pltpu.get_barrier_semaphore()
    for there, place in zip(has, places):

        @pl.when(there)
        def _():
            pl.semaphore_signal(barrier, inc=1, device_id=place, device_id_type=MESH)

    mid[...] = jnp.zeros_like(mid)
    peers = sum(jnp.where(there, jnp.int32(1), jnp.int32(0)) for there in has)
    pl.semaphore_wait(barrier, peers)

    def side_copy(side, k):
        at = pl.ds(HALO + order[k] * LANES, LANES)
        source, target = ((1, strips - 1), (strips - 2, 0))[side]
        return pltpu.make_async_remote_copy(
            src_ref=x.at[source, at, :],
            dst_ref=x.at[target, at, :],
            send_sem=send_side.at[side, k],
            recv_sem=recv_side.at[side, k],
            device_id=places[2 + side],
            device_id_type=MESH,
        )

    def row_copy(side):
        source, target = ((HALO, end), (rows, 0))[side]
        return pltpu.make_async_remote_copy(
            src_ref=x.at[pl.ds(1, strips - 2), pl.ds(source, HALO), :],
            dst_ref=x.at[pl.ds(1, strips - 2), pl.ds(target, HALO), :],
            send_sem=send_row.at[side],
            recv_sem=recv_row.at[side],
            device_id=places[side],
            device_id_type=MESH,
        )

    def end_copy(side, strip):
        source, target = ((HALO, end), (rows, 0))[side]
        b = (0, strips - 1)[strip]
        return pltpu.make_async_remote_copy(
            src_ref=x.at[b, pl.ds(source, HALO), :],
            dst_ref=x.at[b, pl.ds(target, HALO), :],
            send_sem=send_end.at[side, strip],
            recv_sem=recv_end.at[side, strip],
            device_id=places[side],
            device_id_type=MESH,
        )

    local[0].wait()
    local[1].wait()
    for k in range(chunks):
        for side in (0, 1):

            @pl.when(has[2 + side])
            def _():
                side_copy(side, k).start()

    for copy in local[2:]:
        copy.wait()
    for side in (0, 1):

        @pl.when(has[side])
        def _():
            row_copy(side).start()

    for side in (0, 1):

        @pl.when(has[1 - side])
        def _():
            row_copy(side).wait_recv()

    def spread_rows(top, strip_list):
        for b in strip_list:
            if top:
                x[b, 0:HALO, :] = jnp.broadcast_to(x[b, HALO : HALO + 1, :], (HALO, LANES))
            else:
                x[b, end : end + HALO, :] = jnp.broadcast_to(
                    x[b, end - 1 : end, :], (HALO, LANES)
                )

    for top in (0, 1):

        @pl.when(edges[1 - top])
        def _():
            spread_rows(top, range(1, strips - 1))

    tall = rows + 2 * HALO

    @pl.when(edges[2])
    def _():
        x[0, 0:tall, :] = jnp.broadcast_to(x[1, 0:tall, 0:1], (tall, LANES))

    @pl.when(edges[3])
    def _():
        x[strips - 1, 0:tall, :] = jnp.broadcast_to(
            x[strips - 2, 0:tall, LANES - 1 : LANES], (tall, LANES)
        )

    def down(b, carry):
        vertical_pass(x, vhi, vlo, mhi, mlo, b, rows)
        return carry

    lax.fori_loop(1, strips - 1, down, 0)

    def arrival(k):
        for side in (0, 1):

            @pl.when(has[3 - side])
            def _():
                side_copy(side, k).wait_recv()

    arrival(0)
    arrival(1)
    for strip, b in ((0, 0), (1, strips - 1)):

        @pl.when(has[2 + strip])
        def _():
            for side in (0, 1):

                @pl.when(has[side])
                def _():
                    end_copy(side, strip).start()

                @pl.when(edges[side])
                def _():
                    spread_rows(1 - side, (b,))

    for strip in (0, 1):

        @pl.when(has[2 + strip])
        def _():
            for side in (0, 1):

                @pl.when(has[1 - side])
                def _():
                    end_copy(side, strip).wait_recv()

    plan = blocks_of(rows)

    def block(step, carry):
        for k in range(2, chunks):
            at = min(n for n, (need, start) in enumerate(plan) if need > k)

            @pl.when(step == at)
            def _():
                arrival(k)

        start = pick_by(step, [start for need, start in plan])
        for b in (0, strips - 1):
            halo_pass(x, b, start, vhi, vlo, mhi, mlo)
        horizontal_pass(x, vhi, vlo, relief, thi, tlo, mhi, mlo, mid, start, strips)
        return carry

    lax.fori_loop(0, len(plan), block, 0)

    for side in (0, 1):

        @pl.when(has[2 + side])
        def _():
            for k in range(chunks):
                side_copy(side, k).wait_send()

        @pl.when(has[side])
        def _():
            row_copy(side).wait_send()
            for strip in (0, 1):

                @pl.when(has[2 + strip])
                def _():
                    end_copy(side, strip).wait_send()

    repair(relief, strips, HALO, rows, HALO - 8, HALO + rows + 8, edges)
    shade_rows(relief, shade, strips, rows)
    repair(shade, strips, HALO, rows, HALO - 8, HALO + rows + 8, edges)
    outgoing = []

    def send(source, target):
        copy = pltpu.make_async_copy(source, target, sems.at[len(outgoing)])
        copy.start()
        outgoing.append(copy)

    for b in range(strips - 2):
        send(shade.at[b + 1, mine, :], out_shade.at[:, pl.ds(b * LANES, LANES)])

    half, quarter = HALO // 2, HALO // 4
    strips1 = cols // 256 + 2
    low = half - 8

    def keep_first(out, value):
        first[out, low : low + rows // 2 + 16, :] = value

    next_level(shade, strips, low, rows // 2 + 16, range(strips1), uhi, ulo, keep_first)
    repair(first, strips1, half, rows // 2, low, low + rows // 2 + 16, edges)
    for b in range(strips1 - 2):
        send(
            first.at[b + 1, pl.ds(half, rows // 2), :],
            out_first.at[:, pl.ds(b * LANES, LANES)],
        )
    strips2 = cols // 512 + 2
    low2 = quarter - 8

    def keep_second(out, value):
        second[out, low2 : low2 + rows // 4 + 16, :] = value

    next_level(first, strips1, low2, rows // 4 + 16, range(strips2), uhi, ulo, keep_second)
    repair(second, strips2, quarter, rows // 4, low2, low2 + rows // 4 + 16, edges)
    for b in range(strips2 - 2):
        send(
            second.at[b + 1, pl.ds(quarter, rows // 4), :],
            out_second.at[:, pl.ds(b * LANES, LANES)],
        )

    def keep_third(out, value):
        n = min(LANES, cols // 8 - (out - 1) * LANES)
        out_third[(out - 1) * LANES : (out - 1) * LANES + n, :] = value.T[:n, :]

    outs3 = range(1, 1 + -(-cols // 1024))
    next_level(second, strips2, HALO // 8, rows // 8, outs3, uhi, ulo, keep_third)
    for copy in outgoing:
        copy.wait()


def on_device(terrain):
    rows, cols = terrain.shape
    strips = cols // LANES + 2
    chunks = rows // LANES
    f32 = jnp.float32
    tall = rows + 2 * HALO + 8
    anywhere = pl.BlockSpec(memory_space=pl.ANY)
    vmem = pl.BlockSpec(memory_space=pltpu.VMEM)
    shapes = [(rows // k, cols // k) for k in (1, 2, 4)] + [(cols // 8, rows // 8)]
    shade, first, second, third = pl.pallas_call(
        kernel,
        out_shape=tuple(jax.ShapeDtypeStruct(shape, f32) for shape in shapes),
        in_specs=[anywhere],
        out_specs=(anywhere, anywhere, anywhere, vmem),
        scratch_shapes=[
            pltpu.VMEM((strips, tall, LANES), f32),
            pltpu.VMEM((strips, rows + LANES, LANES), f32),
            pltpu.VMEM((strips, rows + LANES, LANES), f32),
            pltpu.VMEM((strips, tall, LANES), f32),
            pltpu.VMEM((strips, tall, LANES), f32),
            pltpu.VMEM((cols // 256 + 2, rows // 2 + HALO, LANES), f32),
            pltpu.VMEM((cols // 512 + 2, rows // 4 + HALO, LANES), f32),
            pltpu.VMEM((strips * LANES + 8, LANES), f32),
            pltpu.VMEM((strips * LANES + 8, LANES), f32),
            pltpu.VMEM((max(tall, strips * LANES), LANES), f32),
            pltpu.VMEM((max(tall, strips * LANES), LANES), f32),
            pltpu.VMEM((strips * LANES, LANES), f32),
            pltpu.VMEM((strips, rows // 2 + 16, LANES), jnp.bfloat16),
            pltpu.VMEM((strips, rows // 2 + 16, LANES), jnp.bfloat16),
            pltpu.SemaphoreType.DMA((2 * strips,)),
            pltpu.SemaphoreType.DMA((2, chunks)),
            pltpu.SemaphoreType.DMA((2, chunks)),
            pltpu.SemaphoreType.DMA((2,)),
            pltpu.SemaphoreType.DMA((2,)),
            pltpu.SemaphoreType.DMA((2, 2)),
            pltpu.SemaphoreType.DMA((2, 2)),
        ],
        compiler_params=pltpu.CompilerParams(
            collective_id=0, has_side_effects=True, vmem_limit_bytes=58 * 1024 * 1024
        ),
    )(terrain)
    return shade, first, second, third.T


def solution(mesh):
    spec = P("rows", "cols")
    return jax.shard_map(
        on_device, mesh=mesh, in_specs=(spec,), out_specs=(spec,) * 4, check_vma=False
    )
```

```python
import math

import jax
import jax.numpy as jnp
from jax import lax
from jax.experimental import pallas as pl
from jax.experimental.pallas import tpu as pltpu
from jax.sharding import PartitionSpec as P

REACH = 120
HALO = 128
LANES = 128
STEPS = 2 * REACH // 8
LIGHT_UP = math.sqrt(0.5)


def rolled(x, k):
    return pltpu.roll(x, x.shape[0] - k, 0)


def group_extremes(load_hi, load_lo, out_hi, out_lo, rows, size=128):
    def body(c, carry):
        r = pl.multiple_of(c * size, 8)
        top = load_hi(r, size + 8)
        if load_lo is None:
            after = rolled(top, 1)
            hi, lo = jnp.maximum(top, after), jnp.minimum(top, after)
        else:
            low = load_lo(r, size + 8)
            hi, lo = jnp.maximum(top, rolled(top, 1)), jnp.minimum(low, rolled(low, 1))
        for k in (2, 4):
            hi = jnp.maximum(hi, rolled(hi, k))
            lo = jnp.minimum(lo, rolled(lo, k))
        out_hi[pl.ds(r, size), :] = hi[:size]
        out_lo[pl.ds(r, size), :] = lo[:size]
        return carry

    lax.fori_loop(0, rows // size, body, 0)


def window_chunk(load, last, pick, groups):
    held = [None] * groups
    run = load(groups - 1)
    for k in range(groups, STEPS):
        run = pick(run, load(k))
    held[groups - 1] = run
    for g in range(groups - 2, -1, -1):
        run = pick(run, load(g))
        held[g] = run
    out = [pick(held[0], last(STEPS))]
    run = None
    for g in range(1, groups):
        nxt = load(g + STEPS - 1)
        run = nxt if run is None else pick(run, nxt)
        out.append(pick(pick(held[g], run), last(g + STEPS)))
    return out


def chunking(groups):
    return max(g for g in range(1, STEPS) if groups % g == 0)


def vertical_pass(x, vhi, vlo, mhi, mlo, b, rows):
    load = lambda r, n: x[b, pl.ds(r, n), :]
    group_extremes(load, None, mhi, mlo, rows + 2 * HALO)
    total = (rows + 16) // 8
    size = chunking(total)

    def body(c, carry):
        base = c * size
        last = lambda k: x[b, pl.ds(pl.multiple_of((base + k) * 8, 8), 8), :]
        for m, v, pick in ((mhi, vhi, jnp.maximum), (mlo, vlo, jnp.minimum)):
            load = lambda k: m[pl.ds(pl.multiple_of((base + k) * 8, 8), 8), :]
            for g, value in enumerate(window_chunk(load, last, pick, size)):
                v[b, pl.ds(pl.multiple_of((base + g) * 8, 8), 8), :] = value
        return carry

    lax.fori_loop(0, total // size, body, 0)


def halo_pass(x, b, start, vhi, vlo, mhi, mlo):
    row = lambda r: pl.multiple_of(start + r, 8)
    span = LANES + 2 * REACH - 8
    load = lambda r, n: x[b, pl.ds(row(r), n), :]
    group_extremes(load, None, mhi, mlo, span, span // 3)
    last = lambda k: x[b, pl.ds(row(k * 8), 8), :]
    for m, v, pick in ((mhi, vhi, jnp.maximum), (mlo, vlo, jnp.minimum)):
        load = lambda k: m[k * 8 : k * 8 + 8, :]
        for g, value in enumerate(window_chunk(load, last, pick, LANES // 8)):
            v[b, pl.ds(row(g * 8), 8), :] = value


def horizontal_pass(x, vhi, vlo, relief, thi, tlo, mhi, mlo, mid, start, strips):
    width = strips * LANES
    r = pl.multiple_of(start, 8)
    for b in range(strips):
        thi[b * LANES : (b + 1) * LANES, :] = vhi[b, pl.ds(r, LANES), :].T
        tlo[b * LANES : (b + 1) * LANES, :] = vlo[b, pl.ds(r, LANES), :].T
    group_extremes(
        lambda s, n: thi[pl.ds(s, n), :], lambda s, n: tlo[pl.ds(s, n), :], mhi, mlo, width
    )
    total = (width - 2 * HALO + 16) // 8
    size = chunking(total)

    def body(c, carry):
        base = c * size
        at = lambda ref: (lambda k: ref[pl.ds(pl.multiple_of((base + k) * 8, 8), 8), :])
        highest = window_chunk(at(mhi), at(thi), jnp.maximum, size)
        lowest = window_chunk(at(mlo), at(tlo), jnp.minimum, size)
        for g in range(size):
            mid[pl.ds(pl.multiple_of(REACH + (base + g) * 8, 8), 8), :] = (
                highest[g] + lowest[g]
            ) * 0.5
        return carry

    lax.fori_loop(0, total // size, body, 0)
    q = pl.multiple_of(r + REACH, 8)
    for b in range(strips):
        relief[b, pl.ds(q, LANES), :] = (
            x[b, pl.ds(q, LANES), :] - mid[b * LANES : (b + 1) * LANES, :].T
        )


def repair(ref, strips, first_row, rows, low, high, edges):
    top, bottom, left, right = edges

    @pl.when(top)
    def _():
        for b in range(strips):
            ref[b, first_row - 8 : first_row, :] = jnp.broadcast_to(
                ref[b, first_row : first_row + 1, :], (8, LANES)
            )

    @pl.when(bottom)
    def _():
        end = first_row + rows
        for b in range(strips):
            ref[b, end : end + 8, :] = jnp.broadcast_to(ref[b, end - 1 : end, :], (8, LANES))

    @pl.when(left)
    def _():
        ref[0, low:high, :] = jnp.broadcast_to(ref[1, low:high, 0:1], (high - low, LANES))

    @pl.when(right)
    def _():
        ref[strips - 1, low:high, :] = jnp.broadcast_to(
            ref[strips - 2, low:high, LANES - 1 : LANES], (high - low, LANES)
        )


def shade_rows(relief, shade, strips, rows):
    size = 16
    width = strips * LANES

    def body(c, carry):
        r = pl.multiple_of(HALO - 16 + c * size, 8)
        wide = jnp.concatenate(
            [relief[b, pl.ds(r - 8, size + 16), :] for b in range(strips)], axis=1
        )
        north = pltpu.roll(wide, 1, 0)[8 : 8 + size]
        south = pltpu.roll(wide, size + 15, 0)[8 : 8 + size]
        here = wide[8 : 8 + size]
        across = north + 2.0 * here + south
        down = south - north
        gx = (pltpu.roll(across, width - 1, 1) - pltpu.roll(across, 1, 1)) * 0.25
        gy = (pltpu.roll(down, width - 1, 1) + 2.0 * down + pltpu.roll(down, 1, 1)) * 0.25
        lit = (LIGHT_UP + 0.5 * gx + 0.5 * gy) * lax.rsqrt(1.0 + gx * gx + gy * gy)
        lit = jnp.maximum(lit, 0.0)
        for b in range(strips):
            shade[b, pl.ds(r, size), :] = lit[:, b * LANES : (b + 1) * LANES]
        return carry

    lax.fori_loop(0, (rows + 32) // size, body, 0)


def tent_matrix(d):
    row = lax.broadcasted_iota(jnp.int32, (LANES, LANES), 0)
    col = lax.broadcasted_iota(jnp.int32, (LANES, LANES), 1)
    t = row + d * LANES - 2 * col + LANES
    near, far = (t == 0) | (t == 1), (t == -1) | (t == 2)
    return jnp.where(near, 0.375, jnp.where(far, 0.125, 0.0)).astype(jnp.bfloat16)


def next_level(source, strips, start, count, outs, uhi, ulo, store):
    def body(b, carry):
        at = lambda k: source[b, pl.ds(2 * start + k, count, stride=2), :]
        u = (at(-1) + at(2)) * 0.125 + (at(0) + at(1)) * 0.375
        upper = u.astype(jnp.bfloat16)
        uhi[b, 0:count, :] = upper
        ulo[b, 0:count, :] = (u - upper.astype(jnp.float32)).astype(jnp.bfloat16)
        return carry

    lax.fori_loop(0, strips, body, 0)
    tents = {d: tent_matrix(d) for d in (-2, -1, 0, 1)}
    for out in outs:
        parts = [b for b in range(2 * out - 2, 2 * out + 2) if 0 <= b < strips]
        weights = jnp.concatenate([tents[b - 2 * out] for b in parts], axis=0)
        total = None
        for u in (uhi, ulo):
            left = jnp.concatenate([u[b, 0:count, :] for b in parts], axis=1)
            term = jnp.dot(left, weights, preferred_element_type=jnp.float32)
            total = term if total is None else total + term
        store(out, total)


def order_of(chunks):
    order = []
    for k in range(chunks // 2):
        order += [chunks - 1 - k, k]
    return order


def blocks_of(rows):
    chunks = rows // LANES
    order = order_of(chunks)
    starts = [k * LANES for k in range(chunks)] + [rows + 16 - LANES]
    plan = []
    for start in starts:
        low, high = start - HALO, start + LANES + 2 * REACH - HALO
        need = {min(max(c, 0), chunks - 1) for c in range(low // LANES, -(-high // LANES))}
        plan.append((max(2, 1 + max(order.index(c) for c in need)), start))
    return sorted(plan)


def pick_by(step, values):
    result = jnp.int32(values[0])
    for k in range(1, len(values)):
        result = jnp.where(step == k, jnp.int32(values[k]), result)
    return result


def kernel(
    own, out_relief, x, vhi, vlo, relief, thi, tlo, mhi, mlo, mid,
    sems, send_side, recv_side, send_row, recv_row, send_end, recv_end,
):
    rows, cols = own.shape
    strips = cols // LANES + 2
    i, ni = lax.axis_index("rows"), lax.axis_size("rows")
    j, nj = lax.axis_index("cols"), lax.axis_size("cols")
    edges = (i == 0, i == ni - 1, j == 0, j == nj - 1)
    has = (i > 0, i < ni - 1, j > 0, j < nj - 1)
    places = ((i - 1, j), (i + 1, j), (i, j - 1), (i, j + 1))
    mine = pl.ds(HALO, rows)
    end = HALO + rows
    chunks = rows // LANES
    order = order_of(chunks)
    MESH = pl.DeviceIdType.MESH

    local = []
    for b in (0, strips - 3, *range(1, strips - 3)):
        copy = pltpu.make_async_copy(
            own.at[:, pl.ds(b * LANES, LANES)], x.at[b + 1, mine, :], sems.at[b]
        )
        copy.start()
        local.append(copy)

    barrier = pltpu.get_barrier_semaphore()
    for there, place in zip(has, places):

        @pl.when(there)
        def _():
            pl.semaphore_signal(barrier, inc=1, device_id=place, device_id_type=MESH)

    mid[...] = jnp.zeros_like(mid)
    peers = sum(jnp.where(there, jnp.int32(1), jnp.int32(0)) for there in has)
    pl.semaphore_wait(barrier, peers)

    def side_copy(side, k):
        at = pl.ds(HALO + order[k] * LANES, LANES)
        source, target = ((1, strips - 1), (strips - 2, 0))[side]
        return pltpu.make_async_remote_copy(
            src_ref=x.at[source, at, :],
            dst_ref=x.at[target, at, :],
            send_sem=send_side.at[side, k],
            recv_sem=recv_side.at[side, k],
            device_id=places[2 + side],
            device_id_type=MESH,
        )

    def row_copy(side):
        source, target = ((HALO, end), (rows, 0))[side]
        return pltpu.make_async_remote_copy(
            src_ref=x.at[pl.ds(1, strips - 2), pl.ds(source, HALO), :],
            dst_ref=x.at[pl.ds(1, strips - 2), pl.ds(target, HALO), :],
            send_sem=send_row.at[side],
            recv_sem=recv_row.at[side],
            device_id=places[side],
            device_id_type=MESH,
        )

    def end_copy(side, strip):
        source, target = ((HALO, end), (rows, 0))[side]
        b = (0, strips - 1)[strip]
        return pltpu.make_async_remote_copy(
            src_ref=x.at[b, pl.ds(source, HALO), :],
            dst_ref=x.at[b, pl.ds(target, HALO), :],
            send_sem=send_end.at[side, strip],
            recv_sem=recv_end.at[side, strip],
            device_id=places[side],
            device_id_type=MESH,
        )

    local[0].wait()
    local[1].wait()
    for k in range(chunks):
        for side in (0, 1):

            @pl.when(has[2 + side])
            def _():
                side_copy(side, k).start()

    for copy in local[2:]:
        copy.wait()
    for side in (0, 1):

        @pl.when(has[side])
        def _():
            row_copy(side).start()

    for side in (0, 1):

        @pl.when(has[1 - side])
        def _():
            row_copy(side).wait_recv()

    def spread_rows(top, strip_list):
        for b in strip_list:
            if top:
                x[b, 0:HALO, :] = jnp.broadcast_to(x[b, HALO : HALO + 1, :], (HALO, LANES))
            else:
                x[b, end : end + HALO, :] = jnp.broadcast_to(
                    x[b, end - 1 : end, :], (HALO, LANES)
                )

    for top in (0, 1):

        @pl.when(edges[1 - top])
        def _():
            spread_rows(top, range(1, strips - 1))

    tall = rows + 2 * HALO

    @pl.when(edges[2])
    def _():
        x[0, 0:tall, :] = jnp.broadcast_to(x[1, 0:tall, 0:1], (tall, LANES))

    @pl.when(edges[3])
    def _():
        x[strips - 1, 0:tall, :] = jnp.broadcast_to(
            x[strips - 2, 0:tall, LANES - 1 : LANES], (tall, LANES)
        )

    def down(b, carry):
        vertical_pass(x, vhi, vlo, mhi, mlo, b, rows)
        return carry

    lax.fori_loop(1, strips - 1, down, 0)

    def arrival(k):
        for side in (0, 1):

            @pl.when(has[3 - side])
            def _():
                side_copy(side, k).wait_recv()

    arrival(0)
    arrival(1)
    for strip, b in ((0, 0), (1, strips - 1)):

        @pl.when(has[2 + strip])
        def _():
            for side in (0, 1):

                @pl.when(has[side])
                def _():
                    end_copy(side, strip).start()

                @pl.when(edges[side])
                def _():
                    spread_rows(1 - side, (b,))

    for strip in (0, 1):

        @pl.when(has[2 + strip])
        def _():
            for side in (0, 1):

                @pl.when(has[1 - side])
                def _():
                    end_copy(side, strip).wait_recv()

    plan = blocks_of(rows)

    def block(step, carry):
        for k in range(2, chunks):
            at = min(n for n, (need, start) in enumerate(plan) if need > k)

            @pl.when(step == at)
            def _():
                arrival(k)

        start = pick_by(step, [start for need, start in plan])
        for b in (0, strips - 1):
            halo_pass(x, b, start, vhi, vlo, mhi, mlo)
        horizontal_pass(x, vhi, vlo, relief, thi, tlo, mhi, mlo, mid, start, strips)
        return carry

    lax.fori_loop(0, len(plan), block, 0)
    some = pl.ds(HALO - 8, rows + 16)
    away = pltpu.make_async_copy(relief.at[:, some, :], out_relief, sems.at[strips])
    away.start()

    for side in (0, 1):

        @pl.when(has[2 + side])
        def _():
            for k in range(chunks):
                side_copy(side, k).wait_send()

        @pl.when(has[side])
        def _():
            row_copy(side).wait_send()
            for strip in (0, 1):

                @pl.when(has[2 + strip])
                def _():
                    end_copy(side, strip).wait_send()

    away.wait()


def finish(
    in_relief, out_shade, out_first, out_second, out_third,
    relief, shade, first, second, uhi, ulo, sems,
):
    rows, cols = out_shade.shape
    strips = cols // LANES + 2
    i, ni = lax.axis_index("rows"), lax.axis_size("rows")
    j, nj = lax.axis_index("cols"), lax.axis_size("cols")
    edges = (i == 0, i == ni - 1, j == 0, j == nj - 1)
    mine = pl.ds(HALO, rows)
    some = pl.ds(HALO - 8, rows + 16)
    fetch = pltpu.make_async_copy(in_relief, relief.at[:, some, :], sems.at[0])
    fetch.start()
    fetch.wait()
    repair(relief, strips, HALO, rows, HALO - 8, HALO + rows + 8, edges)
    shade_rows(relief, shade, strips, rows)
    repair(shade, strips, HALO, rows, HALO - 8, HALO + rows + 8, edges)
    outgoing = []

    def send(source, target):
        copy = pltpu.make_async_copy(source, target, sems.at[len(outgoing)])
        copy.start()
        outgoing.append(copy)

    for b in range(strips - 2):
        send(shade.at[b + 1, mine, :], out_shade.at[:, pl.ds(b * LANES, LANES)])

    half, quarter = HALO // 2, HALO // 4
    strips1 = cols // 256 + 2
    low = half - 8

    def keep_first(out, value):
        first[out, low : low + rows // 2 + 16, :] = value

    next_level(shade, strips, low, rows // 2 + 16, range(strips1), uhi, ulo, keep_first)
    repair(first, strips1, half, rows // 2, low, low + rows // 2 + 16, edges)
    for b in range(strips1 - 2):
        send(
            first.at[b + 1, pl.ds(half, rows // 2), :],
            out_first.at[:, pl.ds(b * LANES, LANES)],
        )
    strips2 = cols // 512 + 2
    low2 = quarter - 8

    def keep_second(out, value):
        second[out, low2 : low2 + rows // 4 + 16, :] = value

    next_level(first, strips1, low2, rows // 4 + 16, range(strips2), uhi, ulo, keep_second)
    repair(second, strips2, quarter, rows // 4, low2, low2 + rows // 4 + 16, edges)
    for b in range(strips2 - 2):
        send(
            second.at[b + 1, pl.ds(quarter, rows // 4), :],
            out_second.at[:, pl.ds(b * LANES, LANES)],
        )

    def keep_third(out, value):
        n = min(LANES, cols // 8 - (out - 1) * LANES)
        out_third[(out - 1) * LANES : (out - 1) * LANES + n, :] = value.T[:n, :]

    outs3 = range(1, 1 + -(-cols // 1024))
    next_level(second, strips2, HALO // 8, rows // 8, outs3, uhi, ulo, keep_third)
    for copy in outgoing:
        copy.wait()


def on_device(terrain):
    rows, cols = terrain.shape
    strips = cols // LANES + 2
    chunks = rows // LANES
    f32 = jnp.float32
    tall = rows + 2 * HALO + 8
    anywhere = pl.BlockSpec(memory_space=pl.ANY)
    vmem = pl.BlockSpec(memory_space=pltpu.VMEM)
    strip = lambda count, tall: pltpu.VMEM((count, tall, LANES), f32)
    params = dict(vmem_limit_bytes=58 * 1024 * 1024)
    relief = pl.pallas_call(
        kernel,
        out_shape=jax.ShapeDtypeStruct((strips, rows + 16, LANES), f32),
        in_specs=[anywhere],
        out_specs=anywhere,
        scratch_shapes=[
            strip(strips, tall),
            strip(strips, rows + LANES),
            strip(strips, rows + LANES),
            strip(strips, tall),
            pltpu.VMEM((strips * LANES + 8, LANES), f32),
            pltpu.VMEM((strips * LANES + 8, LANES), f32),
            pltpu.VMEM((max(tall, strips * LANES), LANES), f32),
            pltpu.VMEM((max(tall, strips * LANES), LANES), f32),
            pltpu.VMEM((strips * LANES, LANES), f32),
            pltpu.SemaphoreType.DMA((2 * strips,)),
            pltpu.SemaphoreType.DMA((2, chunks)),
            pltpu.SemaphoreType.DMA((2, chunks)),
            pltpu.SemaphoreType.DMA((2,)),
            pltpu.SemaphoreType.DMA((2,)),
            pltpu.SemaphoreType.DMA((2, 2)),
            pltpu.SemaphoreType.DMA((2, 2)),
        ],
        compiler_params=pltpu.CompilerParams(
            collective_id=0, has_side_effects=True, **params
        ),
    )(terrain)
    shapes = [(rows // k, cols // k) for k in (1, 2, 4)] + [(cols // 8, rows // 8)]
    shade, first, second, third = pl.pallas_call(
        finish,
        out_shape=tuple(jax.ShapeDtypeStruct(shape, f32) for shape in shapes),
        in_specs=[anywhere],
        out_specs=(anywhere, anywhere, anywhere, vmem),
        scratch_shapes=[
            strip(strips, tall),
            strip(strips, tall),
            strip(cols // 256 + 2, rows // 2 + HALO),
            strip(cols // 512 + 2, rows // 4 + HALO),
            pltpu.VMEM((strips, rows // 2 + 16, LANES), jnp.bfloat16),
            pltpu.VMEM((strips, rows // 2 + 16, LANES), jnp.bfloat16),
            pltpu.SemaphoreType.DMA((2 * strips,)),
        ],
        compiler_params=pltpu.CompilerParams(**params),
    )(relief)
    return shade, first, second, third.T


def solution(mesh):
    spec = P("rows", "cols")
    return jax.shard_map(
        on_device, mesh=mesh, in_specs=(spec,), out_specs=(spec,) * 4, check_vma=False
    )
```
